32 devices in a mesh: gx: 2 (over x), gy: 4 (over z), gz: 4 (over y, core).
Axes of the slice: x: 2, y: 2, z: 4, core: 2. Of those that a mesh axis runs over, the one named last changes fastest.
Arguments:
- populations: float32 [39, 16, 96, 512], P(None, 'gx', 'gy', 'gz'), may hold values from 0.5 to 1.5
- relax: float32 [16, 96, 512], P('gx', 'gy', 'gz'), may hold values from 0.6 to 1.9
Outputs:
- advanced: float32 [39, 16, 96, 512], P(None, 'gx', 'gy', 'gz')
The draws below stay inside these ranges and needn't reach their ends.
All inputs are finite; a program needn't handle non-finite values.
Results may differ from the reference program's by a relative error of at most 0.0001.
Values sent between devices are 32-bit elements; how exact they have to be, the bound alone decides.
No kernel may reach another device: no remote copies, remote signals or barrier semaphores. Data moves between devices by JAX's collectives and lax.ppermute only.
A program may use at most 128 MiB of HBM per device.

```python
import math
import jax
import jax.numpy as jnp

Q = 39
STEPS = 1
NX = 16
NY = 96
NZ = 512


def steps_of(stream_key, shape, cuts, least, high):
    level, own = 1.0, jax.random.fold_in(stream_key, 6)
    for position, blocks in cuts:
        heights = jnp.exp(jax.random.uniform(jax.random.fold_in(own, position), (blocks,), jnp.float32, least / len(cuts), high / len(cuts)))
        level = level * jnp.repeat(heights, shape[position] // blocks).reshape([-1 if axis == position else 1 for axis in range(len(shape))])
    return level


def setup_inputs(seed: int = 0) -> dict:
    splits = jax.random.split(jax.random.key(seed), 3)
    return {
        "populations": jnp.clip(0.5 + 1.0 * jax.random.uniform(splits[0], (Q, NX, NY, NZ), jnp.float32) ** steps_of(splits[0], (Q, NX, NY, NZ), ((1, 2), (2, 4), (3, 4)), -0.2, 0.2), 0.5, 1.5),
        "relax": jnp.clip(jnp.exp(math.log(1.9) - 1.1526795 * jax.random.uniform(splits[1], (NX, NY, NZ), jnp.float32) ** steps_of(splits[1], (NX, NY, NZ), ((0, 2), (1, 4), (2, 4)), -0.2, 0.2)), 0.6, 1.9),
    }


def lattice():
    speeds = [(0, 0, 0)]
    weights = [1.0 / 12.0]
    for axis in range(3):
        for sign in (1, -1):
            vector = [0, 0, 0]
            vector[axis] = sign
            speeds.append(tuple(vector))
            weights.append(1.0 / 12.0)
    for first in (1, -1):
        for second in (1, -1):
            for third in (1, -1):
                speeds.append((first, second, third))
                weights.append(1.0 / 27.0)
    for axis in range(3):
        for sign in (2, -2):
            vector = [0, 0, 0]
            vector[axis] = sign
            speeds.append(tuple(vector))
            weights.append(2.0 / 135.0)
    for couple in ((0, 1), (0, 2), (1, 2)):
        for first in (2, -2):
            for second in (2, -2):
                vector = [0, 0, 0]
                vector[couple[0]] = first
                vector[couple[1]] = second
                speeds.append(tuple(vector))
                weights.append(1.0 / 432.0)
    for axis in range(3):
        for sign in (3, -3):
            vector = [0, 0, 0]
            vector[axis] = sign
            speeds.append(tuple(vector))
            weights.append(1.0 / 1620.0)
    return speeds, weights


def collide(popul, rate):
    speeds, weights = lattice()
    acoustic_wave_rate = 2.0 / 3.0
    inverse = 1.0 / (acoustic_wave_rate ** 0.5)
    zeroth_moment_rho = sum(weights[member] * popul[member] for member in range(39))
    flux = [sum(weights[member] * speeds[member][axis] * popul[member] for member in range(39) if speeds[member][axis] != 0) for axis in range(3)]
    thermal_heat_content = sum(weights[member] * float(sum(value * value for value in speeds[member])) * popul[member] for member in range(1, 39))
    velocity = [part / zeroth_moment_rho for part in flux]
    flow_norm_square = velocity[0] * velocity[0] + velocity[1] * velocity[1] + velocity[2] * velocity[2]
    site_kinetic_heat = (thermal_heat_content / zeroth_moment_rho - flow_norm_square) / (3.0 * acoustic_wave_rate)
    scaled = [part * inverse for part in velocity]
    scaled_square = flow_norm_square / acoustic_wave_rate
    excess_quantity = site_kinetic_heat - 1.0
    results = []
    for member in range(39):
        vector = speeds[member]
        aligned = sum(vector[axis] * inverse * scaled[axis] for axis in range(3) if vector[axis] != 0) if member > 0 else jnp.zeros_like(zeroth_moment_rho)
        speed_square = float(sum(value * value for value in vector)) / acoustic_wave_rate
        aligned_square = aligned * aligned
        hermite = (1.0 + aligned
                   + 0.5 * (aligned_square - scaled_square + excess_quantity * (speed_square - 3.0))
                   + aligned * (aligned_square - 3.0 * scaled_square + 3.0 * excess_quantity * (speed_square - 5.0)) / 6.0
                   + (aligned_square * aligned_square - 6.0 * aligned_square * scaled_square + 3.0 * scaled_square * scaled_square
                      + 6.0 * excess_quantity * (aligned_square * (speed_square - 7.0) + scaled_square * (5.0 - speed_square))
                      + 3.0 * excess_quantity * excess_quantity * (speed_square * speed_square - 10.0 * speed_square + 15.0)) / 24.0)
        maxwellian_target = zeroth_moment_rho * hermite
        results.append(popul[member] - rate * (popul[member] - maxwellian_target))
    return jnp.stack(results)


def reference(populations, relax):
    speeds, weights = lattice()
    state = populations
    for number in range(STEPS):
        post = collide(state, relax)
        state = jnp.stack([jnp.roll(post[member], speeds[member], axis=(0, 1, 2)) for member in range(39)])
    return state
```

```python
import jax
import jax.numpy as jnp
from jax import lax
from jax.experimental import pallas as pl
from jax.experimental.pallas import tpu as pltpu
from jax.sharding import PartitionSpec as P


def lattice():
    speeds = [(0, 0, 0)]
    weights = [1.0 / 12.0]

    def unit(axis, value):
        return tuple(value if axis == other else 0 for other in range(3))

    for axis in range(3):
        for sign in (1, -1):
            speeds.append(unit(axis, sign))
            weights.append(1.0 / 12.0)
    for first in (1, -1):
        for second in (1, -1):
            for third in (1, -1):
                speeds.append((first, second, third))
                weights.append(1.0 / 27.0)
    for axis in range(3):
        for sign in (2, -2):
            speeds.append(unit(axis, sign))
            weights.append(2.0 / 135.0)
    for couple in ((0, 1), (0, 2), (1, 2)):
        for first in (2, -2):
            for second in (2, -2):
                vector = [0, 0, 0]
                vector[couple[0]] = first
                vector[couple[1]] = second
                speeds.append(tuple(vector))
                weights.append(1.0 / 432.0)
    for axis in range(3):
        for sign in (3, -3):
            speeds.append(unit(axis, sign))
            weights.append(1.0 / 1620.0)
    return speeds, weights


SPEEDS, WEIGHTS = lattice()
Q = len(SPEEDS)
OPPOSITE = [SPEEDS.index(tuple(-v for v in c)) for c in SPEEDS]
PAIRS = [(m, OPPOSITE[m]) for m in range(Q) if m < OPPOSITE[m]]
F32 = jnp.float32

ZOFF = {}
_next = 0
for _sign in (1, -1):
    for _m in range(Q):
        if SPEEDS[_m][2] * _sign > 0:
            ZOFF[_m] = _next
            _next += abs(SPEEDS[_m][2])
ZHALF = _next // 2

XOFF = {}
_next = 0
for _sign in (1, -1):
    for _m in range(Q):
        if SPEEDS[_m][0] * _sign > 0:
            XOFF[_m] = _next
            _next += abs(SPEEDS[_m][0])
XHALF = _next // 2

YOFF = {}
for _sign in (1, -1):
    _next = 0
    for _m in range(Q):
        if SPEEDS[_m][1] * _sign > 0:
            YOFF[_m] = _next
            _next += abs(SPEEDS[_m][1])
YCOUNT = _next

EOFF = {}
_next = 0
for _sign in (1, -1):
    for _m in range(Q):
        if SPEEDS[_m][0] * _sign > 0 and SPEEDS[_m][1] != 0:
            EOFF[_m] = _next
            _next += abs(SPEEDS[_m][0]) * abs(SPEEDS[_m][1])
ECOUNT = _next


def wrapped_rows(speed, count):
    return range(speed) if speed > 0 else range(count + speed, count)


def z_home(member, lanes):
    speed = SPEEDS[member][2]
    lane = lax.broadcasted_iota(jnp.int32, (1, lanes), 1)
    if speed > 0:
        return (-ZOFF[member]) % lanes, lane < speed
    return (lanes + speed - ZOFF[member]) % lanes, lane >= lanes + speed


def collide_rows(load, rate, store):
    total = load(0)
    groups = {}
    flux = [None, None, None]

    def add(old, new):
        return new if old is None else old + new

    acc = {}
    for m, n in PAIRS:
        c = SPEEDS[m]
        s = sum(v * v for v in c)
        gm, gn = load(m), load(n)
        groups[s] = add(groups.get(s), gm + gn)
        diff = gm - gn
        for axis in range(3):
            if c[axis]:
                key = (s, axis)
                part = diff if c[axis] > 0 else -diff
                acc[key] = part if key not in acc else (acc[key] + diff if c[axis] > 0 else acc[key] - diff)
        groups[("w", s)] = WEIGHTS[m]
        groups[("c", s)] = max(abs(v) for v in c)
    squares = sorted(k for k in groups if not isinstance(k, tuple))
    rho = WEIGHTS[0] * total
    energy = None
    for s in squares:
        part = groups[("w", s)] * groups[s]
        rho = rho + part
        energy = add(energy, float(s) * part)
        for axis in range(3):
            flux[axis] = add(flux[axis], (groups[("w", s)] * groups[("c", s)]) * acc[(s, axis)])
    cs2 = 2.0 / 3.0
    inv = 1.0 / rho
    u = [f * inv for f in flux]
    uu = u[0] * u[0] + u[1] * u[1] + u[2] * u[2]
    t = (energy * inv - uu) * (1.0 / (3.0 * cs2)) - 1.0
    b = uu * (1.0 / cs2)
    scale = rate * rho
    keep = 1.0 - rate
    w = [part * (1.0 / cs2) for part in u]
    fourth = scale * (1.0 / 24.0)
    third = scale * (1.0 / 6.0)
    bb = b * b * 0.125
    tt = t * t * 0.125
    tb = t * b * 0.25
    coeff = {}
    for s in [0] + squares:
        e = s / cs2
        k = scale * (1.0 - 0.5 * b + t * (0.5 * (e - 3.0)) + bb + tb * (5.0 - e) + tt * (e * e - 10.0 * e + 15.0))
        if s:
            l = scale * (0.5 - 0.25 * b + t * (0.25 * (e - 7.0)))
            q = scale * (1.0 - 0.5 * b + t * (0.5 * (e - 5.0)))
            coeff[s] = (k, l, q)
        else:
            coeff[s] = (k,)
    store(0, keep * total + coeff[0][0])
    for m, n in PAIRS:
        c = SPEEDS[m]
        s = sum(v * v for v in c)
        k, l, q = coeff[s]
        a = None
        for axis in range(3):
            if c[axis]:
                if a is None:
                    a = w[axis] if c[axis] > 0 else -w[axis]
                else:
                    a = a + w[axis] if c[axis] > 0 else a - w[axis]
        size = max(abs(v) for v in c)
        if size != 1:
            a = a * float(size)
        aa = a * a
        even = k + aa * (l + aa * fourth)
        odd = a * (q + aa * third)
        store(m, keep * load(m) + (even + odd))
        store(n, keep * load(n) + (even - odd))


def collide_kernel(g_ref, r_ref, w_ref, xs_ref, y_up_ref, y_down_ref, z_ref, s_ref, *, nx, ny, nz, depth):
    step = pl.program_id(0)
    lane = lax.broadcasted_iota(jnp.int32, (1, nz), 1)
    for i in range(depth):
        x = step * depth + i

        def chunk(j, i=i):
            row = j * 8

            def load(m):
                return g_ref[m, i, row : row + 8, :]

            def store(m, value):
                s_ref[m, 8 + row : 16 + row, :] = value
                if SPEEDS[m][1] != 0:
                    if j == 0:
                        s_ref[m, 8 + ny : 16 + ny, :] = value
                    if j == ny // 8 - 1:
                        s_ref[m, 0:8, :] = value

            collide_rows(load, r_ref[i, row : row + 8, :], store)

        for j in range(ny // 8):
            chunk(j)
        packed = jnp.zeros((ny, nz), F32)
        for m in list(range(Q - 1, -1, -1)):
            cx, cy, cz = SPEEDS[m]
            value = s_ref[m, 8 - cy : 8 - cy + ny, :]
            if cz:
                size = abs(cz)
                shift = (cz + ZOFF[m]) % nz if cz > 0 else ZOFF[m]
                inside = (lane >= ZOFF[m]) & (lane < ZOFF[m] + size)
                packed = jnp.where(inside, pltpu.roll(value, shift, 1) if shift else value, packed)
                value = pltpu.roll(value, cz % nz, 1)
            target = lax.rem(x + cx + nx, nx)
            w_ref[m, target] = value
            if cx:
                size = abs(cx)
                up = m if cx > 0 else OPPOSITE[m]
                slot = XOFF[up] + lax.rem(x + (size - nx % size), size)
                if cx < 0:
                    slot = jnp.where(x < size, XOFF[m] + x, slot)
                xs_ref[slot] = value
            if cy:
                ref = y_up_ref if cy > 0 else y_down_ref
                for k, row in enumerate(wrapped_rows(cy, ny)):
                    ref[YOFF[m] + k, pl.ds(x, 1), :] = value[row : row + 1, :]
        z_ref[x] = packed


def z_edge_kernel(z_low_ref, z_high_ref, y_up_ref, y_down_ref, z_out, y_up_out, y_down_out, *, nx, ny, nz):
    lane = lax.broadcasted_iota(jnp.int32, (1, 1, nz), 2)
    z_out[...] = jnp.where(lane < ZHALF, z_low_ref[...], z_high_ref[...])
    for m in range(Q):
        cx, cy, cz = SPEEDS[m]
        if not cy:
            continue
        source, out = (y_up_ref, y_up_out) if cy > 0 else (y_down_ref, y_down_out)
        for k, row in enumerate(wrapped_rows(cy, ny)):
            value = source[YOFF[m] + k]
            if cz:
                shift, mask = z_home(m, nz)
                ref = z_low_ref if cz > 0 else z_high_ref
                halo = ref[:, row, :]
                value = jnp.where(mask, pltpu.roll(halo, shift, 1) if shift else halo, value)
            out[YOFF[m] + k] = value


def y_edge_kernel(z_ref, y_low_ref, y_high_ref, out_ref, *, nx, ny, nz):
    out_ref[0:2] = z_ref[nx - 2 : nx]
    out_ref[2:4] = z_ref[0:2]
    for m, base in EOFF.items():
        cx, cy, _ = SPEEDS[m]
        size = abs(cx)
        ref = y_low_ref if cy > 0 else y_high_ref
        for k in range(abs(cy)):
            first = base + k * size
            start = nx - size if cx > 0 else 0
            out_ref[4 + first // ny, first % ny : first % ny + size, :] = ref[YOFF[m] + k, start : start + size, :]


def finish_kernel(w_ref, xr_ref, z_ref, y_low_ref, y_high_ref, edge_ref, out_ref, *, nx, ny, nz, depth):
    step = pl.program_id(0)
    for i in range(depth):
        x = step * depth + i
        for m in range(Q):
            cx, cy, cz = SPEEDS[m]
            size = abs(cx)
            source = lax.rem(x - cx + nx, nx)
            value = w_ref[m, i]
            if cx > 0:
                crossed = x < size
                layer = jnp.where(crossed, x, 0)
            elif cx < 0:
                crossed = x >= nx - size
                layer = jnp.where(crossed, x - (nx - size), 0)
            if cx:
                value = jnp.where(crossed, xr_ref[XOFF[m] + layer], value)
            if cz:
                halo = z_ref[source]
                if cx:
                    base = 2 - size if cx > 0 else 2
                    halo = jnp.where(crossed, edge_ref[base + layer], halo)
                shift, mask = z_home(m, nz)
                value = jnp.where(mask, pltpu.roll(halo, shift, 1) if shift else halo, value)
            out_ref[m, i] = value
            if cy:
                ref = y_low_ref if cy > 0 else y_high_ref
                for k, row in enumerate(wrapped_rows(cy, ny)):
                    line = ref[YOFF[m] + k, pl.ds(source, 1), :]
                    if cx:
                        first = EOFF[m] + k * size
                        other = edge_ref[4 + first // ny, pl.ds(first % ny + layer, 1), :]
                        line = jnp.where(crossed, other, line)
                    out_ref[m, i, row : row + 1, :] = line


def from_behind(block, axis, distance):
    count = lax.axis_size(axis)
    route = [((i - distance) % count, i) for i in range(count)]
    return lax.ppermute(block, axis, route)


def params(steps=0):
    if steps:
        return pltpu.CompilerParams(dimension_semantics=("arbitrary",), vmem_limit_bytes=50 * 1024 * 1024)
    return pltpu.CompilerParams(vmem_limit_bytes=50 * 1024 * 1024)


def whole(shape):
    return pl.BlockSpec(shape, lambda s: (0,) * len(shape))


def per_device(populations, relax):
    _, nx, ny, nz = populations.shape
    dims = dict(nx=nx, ny=ny, nz=nz)
    depth = 2 if nx % 2 == 0 else 1
    steps = nx // depth

    def struct(*shape):
        return jax.ShapeDtypeStruct(shape, F32)

    field = struct(Q, nx, ny, nz)
    xs = struct(2 * XHALF, ny, nz)
    ys = struct(YCOUNT, nx, nz)
    zs = struct(nx, ny, nz)
    edge = struct(4 + -(-ECOUNT // ny), ny, nz)
    cells = nx * ny * nz

    import functools

    state, x_send, y_up, y_down, z_send = pl.pallas_call(
        functools.partial(collide_kernel, depth=depth, **dims),
        grid=(steps,),
        in_specs=[
            pl.BlockSpec((Q, depth, ny, nz), lambda s: (0, s, 0, 0)),
            pl.BlockSpec((depth, ny, nz), lambda s: (s, 0, 0)),
        ],
        out_specs=[whole(a.shape) for a in (field, xs, ys, ys, zs)],
        out_shape=[field, xs, ys, ys, zs],
        scratch_shapes=[pltpu.VMEM((Q, ny + 16, nz), F32)],
        compiler_params=params(steps),
        name="collide",
    )(populations, relax)

    if lax.axis_size("gx") == 2:
        x_recv = from_behind(x_send, "gx", 1)
    else:
        x_recv = jnp.concatenate(
            [from_behind(x_send[:XHALF], "gx", 1), from_behind(x_send[XHALF:], "gx", -1)]
        )
    z_low = from_behind(z_send, "gz", 1)
    z_high = from_behind(z_send, "gz", -1)
    z_all, y_up, y_down = pl.pallas_call(
        functools.partial(z_edge_kernel, **dims),
        out_shape=[zs, ys, ys],
        compiler_params=params(),
        name="z_edge",
    )(z_low, z_high, y_up, y_down)
    y_low = from_behind(y_up, "gy", 1)
    y_high = from_behind(y_down, "gy", -1)
    edge_send = pl.pallas_call(
        functools.partial(y_edge_kernel, **dims),
        out_shape=edge,
        compiler_params=params(),
        name="y_edge",
    )(z_all, y_low, y_high)
    if lax.axis_size("gx") == 2:
        edge_recv = from_behind(edge_send, "gx", 1)
    else:
        lower = from_behind(edge_send, "gx", 1)
        upper = from_behind(edge_send, "gx", -1)
        layer = lax.broadcasted_iota(jnp.int32, edge.shape, 0)
        line = (layer - 4) * ny + lax.broadcasted_iota(jnp.int32, edge.shape, 1)
        is_low = jnp.where(layer < 4, layer < 2, line < ECOUNT // 2)
        edge_recv = jnp.where(is_low, lower, upper)
    return pl.pallas_call(
        functools.partial(finish_kernel, depth=depth, **dims),
        grid=(steps,),
        in_specs=[
            pl.BlockSpec((Q, depth, ny, nz), lambda s: (0, s, 0, 0)),
            whole(xs.shape),
            whole(zs.shape),
            whole(ys.shape),
            whole(ys.shape),
            whole(edge.shape),
        ],
        out_specs=pl.BlockSpec((Q, depth, ny, nz), lambda s: (0, s, 0, 0)),
        out_shape=field,
        compiler_params=params(steps),
        name="finish",
    )(state, x_recv, z_all, y_low, y_high, edge_recv)


def solution(mesh):
    return jax.shard_map(
        per_device,
        mesh=mesh,
        in_specs=(P(None, "gx", "gy", "gz"), P("gx", "gy", "gz")),
        out_specs=P(None, "gx", "gy", "gz"),
        check_vma=False,
    )
```

```python
import functools

import jax
import jax.numpy as jnp
from jax import lax
from jax.experimental import pallas as pl
from jax.experimental.pallas import tpu as pltpu
from jax.sharding import PartitionSpec as P


def lattice():
    speeds = [(0, 0, 0)]
    weights = [1.0 / 12.0]

    def unit(axis, value):
        return tuple(value if axis == other else 0 for other in range(3))

    for axis in range(3):
        for sign in (1, -1):
            speeds.append(unit(axis, sign))
            weights.append(1.0 / 12.0)
    for first in (1, -1):
        for second in (1, -1):
            for third in (1, -1):
                speeds.append((first, second, third))
                weights.append(1.0 / 27.0)
    for axis in range(3):
        for sign in (2, -2):
            speeds.append(unit(axis, sign))
            weights.append(2.0 / 135.0)
    for couple in ((0, 1), (0, 2), (1, 2)):
        for first in (2, -2):
            for second in (2, -2):
                vector = [0, 0, 0]
                vector[couple[0]] = first
                vector[couple[1]] = second
                speeds.append(tuple(vector))
                weights.append(1.0 / 432.0)
    for axis in range(3):
        for sign in (3, -3):
            speeds.append(unit(axis, sign))
            weights.append(1.0 / 1620.0)
    return speeds, weights


SPEEDS, WEIGHTS = lattice()
Q = len(SPEEDS)
OPPOSITE = [SPEEDS.index(tuple(-v for v in c)) for c in SPEEDS]
PAIRS = [(m, OPPOSITE[m]) for m in range(Q) if m < OPPOSITE[m]]
F32 = jnp.float32

ZOFF = {}
_next = 0
for _sign in (1, -1):
    for _m in range(Q):
        if SPEEDS[_m][2] * _sign > 0:
            ZOFF[_m] = _next
            _next += abs(SPEEDS[_m][2])
ZHALF = _next // 2

XOFF = {}
_next = 0
for _sign in (1, -1):
    for _m in range(Q):
        if SPEEDS[_m][0] * _sign > 0:
            XOFF[_m] = _next
            _next += abs(SPEEDS[_m][0])
XHALF = _next // 2

YOFF = {}
for _sign in (1, -1):
    _next = 0
    for _m in range(Q):
        if SPEEDS[_m][1] * _sign > 0:
            YOFF[_m] = _next
            _next += abs(SPEEDS[_m][1])
YCOUNT = _next

EOFF = {}
_next = 0
for _sign in (1, -1):
    for _m in range(Q):
        if SPEEDS[_m][0] * _sign > 0 and SPEEDS[_m][1] != 0:
            EOFF[_m] = _next
            _next += abs(SPEEDS[_m][0]) * abs(SPEEDS[_m][1])
ECOUNT = _next


def wrapped_rows(speed, count):
    return range(speed) if speed > 0 else range(count + speed, count)


def z_home(member, lanes):
    speed = SPEEDS[member][2]
    lane = lax.broadcasted_iota(jnp.int32, (1, lanes), 1)
    if speed > 0:
        return (-ZOFF[member]) % lanes, lane < speed
    return (lanes + speed - ZOFF[member]) % lanes, lane >= lanes + speed


def collide_rows(load, rate, store):
    total = load(0)
    groups = {}
    flux = [None, None, None]

    def add(old, new):
        return new if old is None else old + new

    acc = {}
    for m, n in PAIRS:
        c = SPEEDS[m]
        s = sum(v * v for v in c)
        gm, gn = load(m), load(n)
        groups[s] = add(groups.get(s), gm + gn)
        diff = gm - gn
        for axis in range(3):
            if c[axis]:
                key = (s, axis)
                part = diff if c[axis] > 0 else -diff
                acc[key] = part if key not in acc else (acc[key] + diff if c[axis] > 0 else acc[key] - diff)
        groups[("w", s)] = WEIGHTS[m]
        groups[("c", s)] = max(abs(v) for v in c)
    squares = sorted(k for k in groups if not isinstance(k, tuple))
    rho = WEIGHTS[0] * total
    energy = None
    for s in squares:
        part = groups[("w", s)] * groups[s]
        rho = rho + part
        energy = add(energy, float(s) * part)
        for axis in range(3):
            flux[axis] = add(flux[axis], (groups[("w", s)] * groups[("c", s)]) * acc[(s, axis)])
    cs2 = 2.0 / 3.0
    inv = 1.0 / rho
    u = [f * inv for f in flux]
    uu = u[0] * u[0] + u[1] * u[1] + u[2] * u[2]
    t = (energy * inv - uu) * (1.0 / (3.0 * cs2)) - 1.0
    b = uu * (1.0 / cs2)
    scale = rate * rho
    keep = 1.0 - rate
    w = [part * (1.0 / cs2) for part in u]
    fourth = scale * (1.0 / 24.0)
    third = scale * (1.0 / 6.0)
    bb = b * b * 0.125
    tt = t * t * 0.125
    tb = t * b * 0.25
    coeff = {}
    for s in [0] + squares:
        e = s / cs2
        k = scale * (1.0 - 0.5 * b + t * (0.5 * (e - 3.0)) + bb + tb * (5.0 - e) + tt * (e * e - 10.0 * e + 15.0))
        if s:
            l = scale * (0.5 - 0.25 * b + t * (0.25 * (e - 7.0)))
            q = scale * (1.0 - 0.5 * b + t * (0.5 * (e - 5.0)))
            coeff[s] = (k, l, q)
        else:
            coeff[s] = (k,)
    store(0, keep * total + coeff[0][0])
    for m, n in PAIRS:
        c = SPEEDS[m]
        s = sum(v * v for v in c)
        k, l, q = coeff[s]
        a = None
        for axis in range(3):
            if c[axis]:
                if a is None:
                    a = w[axis] if c[axis] > 0 else -w[axis]
                else:
                    a = a + w[axis] if c[axis] > 0 else a - w[axis]
        size = max(abs(v) for v in c)
        if size != 1:
            a = a * float(size)
        aa = a * a
        even = k + aa * (l + aa * fourth)
        odd = a * (q + aa * third)
        store(m, keep * load(m) + (even + odd))
        store(n, keep * load(n) + (even - odd))


def collide_kernel(g_ref, r_ref, w_ref, xs_ref, y_up_ref, y_down_ref, z_ref, s_ref, *, nx, ny, nz, depth):
    step = pl.program_id(0)
    lane = lax.broadcasted_iota(jnp.int32, (1, nz), 1)
    for i in range(depth):
        x = step * depth + i

        def chunk(j, i=i):
            row = j * 8

            def load(m):
                return g_ref[m, i, row : row + 8, :]

            def store(m, value):
                s_ref[m, 8 + row : 16 + row, :] = value
                if SPEEDS[m][1] != 0:
                    if j == 0:
                        s_ref[m, 8 + ny : 16 + ny, :] = value
                    if j == ny // 8 - 1:
                        s_ref[m, 0:8, :] = value

            collide_rows(load, r_ref[i, row : row + 8, :], store)

        for j in range(ny // 8):
            chunk(j)
        packed = jnp.zeros((ny, nz), F32)
        for m in list(range(Q - 1, -1, -1)):
            cx, cy, cz = SPEEDS[m]
            value = s_ref[m, 8 - cy : 8 - cy + ny, :]
            if cz:
                size = abs(cz)
                shift = (cz + ZOFF[m]) % nz if cz > 0 else ZOFF[m]
                inside = (lane >= ZOFF[m]) & (lane < ZOFF[m] + size)
                packed = jnp.where(inside, pltpu.roll(value, shift, 1) if shift else value, packed)
                value = pltpu.roll(value, cz % nz, 1)
            target = lax.rem(x + cx + nx, nx)
            w_ref[m, target] = value
            if cx:
                size = abs(cx)
                up = m if cx > 0 else OPPOSITE[m]
                slot = XOFF[up] + lax.rem(x + (size - nx % size), size)
                if cx < 0:
                    slot = jnp.where(x < size, XOFF[m] + x, slot)
                xs_ref[slot] = value
            if cy:
                ref = y_up_ref if cy > 0 else y_down_ref
                for k, row in enumerate(wrapped_rows(cy, ny)):
                    ref[YOFF[m] + k, pl.ds(x, 1), :] = value[row : row + 1, :]
        z_ref[x] = packed


def z_edge_kernel(z_low_ref, z_high_ref, y_up_ref, y_down_ref, z_out, y_up_out, y_down_out, *, nx, ny, nz):
    lane = lax.broadcasted_iota(jnp.int32, (1, 1, nz), 2)
    z_out[...] = jnp.where(lane < ZHALF, z_low_ref[...], z_high_ref[...])
    for m in range(Q):
        cx, cy, cz = SPEEDS[m]
        if not cy:
            continue
        source, out = (y_up_ref, y_up_out) if cy > 0 else (y_down_ref, y_down_out)
        for k, row in enumerate(wrapped_rows(cy, ny)):
            value = source[YOFF[m] + k]
            if cz:
                shift, mask = z_home(m, nz)
                ref = z_low_ref if cz > 0 else z_high_ref
                halo = ref[:, row, :]
                value = jnp.where(mask, pltpu.roll(halo, shift, 1) if shift else halo, value)
            out[YOFF[m] + k] = value


def y_edge_kernel(z_ref, y_low_ref, y_high_ref, out_ref, *, nx, ny, nz):
    out_ref[0:2] = z_ref[nx - 2 : nx]
    out_ref[2:4] = z_ref[0:2]
    for m, base in EOFF.items():
        cx, cy, _ = SPEEDS[m]
        size = abs(cx)
        ref = y_low_ref if cy > 0 else y_high_ref
        for k in range(abs(cy)):
            first = base + k * size
            start = nx - size if cx > 0 else 0
            out_ref[4 + first // ny, first % ny : first % ny + size, :] = ref[YOFF[m] + k, start : start + size, :]


def inner_kernel(w_ref, z_ref, y_low_ref, y_high_ref, out_ref, *, nx, ny, nz, depth):
    step = pl.program_id(0)
    for i in range(depth):
        x = step * depth + i
        for m in range(Q):
            cx, cy, cz = SPEEDS[m]
            source = lax.rem(x - cx + nx, nx)
            value = w_ref[m, i]
            if cz:
                halo = z_ref[source]
                shift, mask = z_home(m, nz)
                value = jnp.where(mask, pltpu.roll(halo, shift, 1) if shift else halo, value)
            out_ref[m, i] = value
            if cy:
                ref = y_low_ref if cy > 0 else y_high_ref
                for k, row in enumerate(wrapped_rows(cy, ny)):
                    out_ref[m, i, row : row + 1, :] = ref[YOFF[m] + k, pl.ds(source, 1), :]


def outer_kernel(inner_ref, xr_ref, edge_ref, out_ref, layers_ref, sems, *, nx, ny, nz):
    copies = []
    for m, slot in XOFF.items():
        cx, cy, cz = SPEEDS[m]
        size = abs(cx)
        plain = cy == 0 and cz == 0
        if not plain:
            for layer in range(size):
                value = xr_ref[slot + layer]
                if cz:
                    halo = edge_ref[(2 - size if cx > 0 else 2) + layer]
                    shift, mask = z_home(m, nz)
                    value = jnp.where(mask, pltpu.roll(halo, shift, 1) if shift else halo, value)
                layers_ref[slot + layer] = value
                if cy:
                    for k, row in enumerate(wrapped_rows(cy, ny)):
                        line = EOFF[m] + k * size + layer
                        at = (4 + line // ny, slice(line % ny, line % ny + 1))
                        layers_ref[slot + layer, row : row + 1, :] = edge_ref[at[0], at[1], :]
        start = 0 if cx > 0 else nx - size
        copy = pltpu.make_async_copy(
            (xr_ref if plain else layers_ref).at[pl.ds(slot, size)],
            out_ref.at[m, pl.ds(start, size)],
            sems.at[len(copies)],
        )
        copy.start()
        copies.append(copy)
    for copy in copies:
        copy.wait()


def from_behind(block, axis, distance):
    count = lax.axis_size(axis)
    route = [((i - distance) % count, i) for i in range(count)]
    return lax.ppermute(block, axis, route)


def params(steps=0):
    if steps:
        return pltpu.CompilerParams(dimension_semantics=("arbitrary",), vmem_limit_bytes=50 * 1024 * 1024)
    return pltpu.CompilerParams(vmem_limit_bytes=50 * 1024 * 1024)


def whole(shape):
    return pl.BlockSpec(shape, lambda s: (0,) * len(shape))


def per_device(populations, relax):
    _, nx, ny, nz = populations.shape
    dims = dict(nx=nx, ny=ny, nz=nz)
    depth = 2 if nx % 2 == 0 else 1
    steps = nx // depth

    def struct(*shape):
        return jax.ShapeDtypeStruct(shape, F32)

    field = struct(Q, nx, ny, nz)
    xs = struct(2 * XHALF, ny, nz)
    ys = struct(YCOUNT, nx, nz)
    zs = struct(nx, ny, nz)
    edge = struct(4 + -(-ECOUNT // ny), ny, nz)
    cells = nx * ny * nz

    state, x_send, y_up, y_down, z_send = pl.pallas_call(
        functools.partial(collide_kernel, depth=depth, **dims),
        grid=(steps,),
        in_specs=[
            pl.BlockSpec((Q, depth, ny, nz), lambda s: (0, s, 0, 0)),
            pl.BlockSpec((depth, ny, nz), lambda s: (s, 0, 0)),
        ],
        out_specs=[whole(a.shape) for a in (field, xs, ys, ys, zs)],
        out_shape=[field, xs, ys, ys, zs],
        scratch_shapes=[pltpu.VMEM((Q, ny + 16, nz), F32)],
        compiler_params=params(steps),
        name="collide",
    )(populations, relax)

    if lax.axis_size("gx") == 2:
        x_recv = from_behind(x_send, "gx", 1)
    else:
        x_recv = jnp.concatenate(
            [from_behind(x_send[:XHALF], "gx", 1), from_behind(x_send[XHALF:], "gx", -1)]
        )
    z_low = from_behind(z_send, "gz", 1)
    z_high = from_behind(z_send, "gz", -1)
    z_all, y_up, y_down = pl.pallas_call(
        functools.partial(z_edge_kernel, **dims),
        out_shape=[zs, ys, ys],
        compiler_params=params(),
        name="z_edge",
    )(z_low, z_high, y_up, y_down)
    y_low = from_behind(y_up, "gy", 1)
    y_high = from_behind(y_down, "gy", -1)
    edge_send = pl.pallas_call(
        functools.partial(y_edge_kernel, **dims),
        out_shape=edge,
        compiler_params=params(),
        name="y_edge",
    )(z_all, y_low, y_high)
    if lax.axis_size("gx") == 2:
        edge_recv = from_behind(edge_send, "gx", 1)
    else:
        lower = from_behind(edge_send, "gx", 1)
        upper = from_behind(edge_send, "gx", -1)
        layer = lax.broadcasted_iota(jnp.int32, edge.shape, 0)
        line = (layer - 4) * ny + lax.broadcasted_iota(jnp.int32, edge.shape, 1)
        is_low = jnp.where(layer < 4, layer < 2, line < ECOUNT // 2)
        edge_recv = jnp.where(is_low, lower, upper)
    inner = pl.pallas_call(
        functools.partial(inner_kernel, depth=depth, **dims),
        grid=(steps,),
        in_specs=[
            pl.BlockSpec((Q, depth, ny, nz), lambda s: (0, s, 0, 0)),
            whole(zs.shape),
            whole(ys.shape),
            whole(ys.shape),
        ],
        out_specs=pl.BlockSpec((Q, depth, ny, nz), lambda s: (0, s, 0, 0)),
        out_shape=field,
        compiler_params=params(steps),
        cost_estimate=pl.CostEstimate(flops=400 * cells, bytes_accessed=8 * Q * cells, transcendentals=0),
        name="inner",
    )(state, z_all, y_low, y_high)
    return pl.pallas_call(
        functools.partial(outer_kernel, **dims),
        in_specs=[
            pl.BlockSpec(memory_space=pl.ANY),
            pl.BlockSpec(memory_space=pltpu.VMEM),
            pl.BlockSpec(memory_space=pltpu.VMEM),
        ],
        out_specs=pl.BlockSpec(memory_space=pl.ANY),
        out_shape=field,
        input_output_aliases={0: 0},
        scratch_shapes=[pltpu.VMEM(xs.shape, F32), pltpu.SemaphoreType.DMA((len(XOFF),))],
        compiler_params=params(),
        name="outer",
    )(inner, x_recv, edge_recv)


def solution(mesh):
    return jax.shard_map(
        per_device,
        mesh=mesh,
        in_specs=(P(None, "gx", "gy", "gz"), P("gx", "gy", "gz")),
        out_specs=P(None, "gx", "gy", "gz"),
        check_vma=False,
    )
```
